32 devices in a mesh: dop: 2 (over core), tm: 16 (over z, y, x).
Axes of the slice: x: 2, y: 2, z: 4, core: 2. Of those that a mesh axis runs over, the one named last changes fastest.
Arguments:
- surveillance: bfloat16 [2, 16, 8192], P(None, 'tm', 'dop'), may hold values from -6 to 6
- reference_signal: bfloat16 [2, 16, 8192], P(None, 'tm', 'dop'), may hold values from -6 to 6
Outputs:
- ambiguity: float32 [2048, 2, 512], P('tm', None, 'dop')
The draws below stay inside these ranges and needn't reach their ends.
All inputs are finite; a program needn't handle non-finite values.
Results may differ from the reference program's by a relative error of at most 0.0029.
Values may be sent and summed in bfloat16 or wider, within the bound.
A program may use at most 128 MiB of HBM per device.

```python
import math
import jax
import jax.numpy as jnp
from jax import lax

F = 512
LAGS = 2048
BLOCK = 8192
BLOCKS = 16
TIME = 131072


def levels(own_key, extent, split, least, high):
    loudness = 1.0
    for axis_at, shards_of in split:
        heights = jax.random.uniform(jax.random.fold_in(jax.random.fold_in(own_key, 6), axis_at), (shards_of,), jnp.float32, least / len(split), high / len(split))
        loudness = loudness * jnp.repeat(jnp.exp(heights), extent[axis_at] // shards_of).reshape((-1,) + (1,) * (len(extent) - 1 - axis_at))
    return loudness


def scatter_about(rng, extent, spread, limit, split=(), held_as=jnp.bfloat16):
    entries = spread * jax.random.normal(rng, extent, jnp.float32)
    if split:
        entries = entries * levels(rng, extent, split, -0.22, 0.18)
    return jnp.clip(entries, -limit, limit).astype(held_as)


def setup_inputs(seed: int = 0) -> dict:
    splits = jax.random.split(jax.random.key(seed), 3)
    return {
        "surveillance": scatter_about(splits[0], (2, BLOCKS, BLOCK), 1.0, 6.0, ((1, 16), (2, 2))),
        "reference_signal": scatter_about(splits[1], (2, BLOCKS, BLOCK), 1.0, 6.0, ((1, 16), (2, 2))),
    }


def toeplitz_rows(segment, height, breadth):
    length = height + breadth - 1
    repeated = jnp.tile(segment, (1, height + 1))[:, :height * (length + 1)]
    return repeated.reshape(2, height, length + 1)[:, :, :breadth]

def mix_rows(samples, sample_index, doppler, window):
    phase_step = jnp.mod(doppler[:, None] * sample_index[None, :], window)
    phase_angle = phase_step.astype(jnp.float32) * (2.0 * math.pi / window)
    cosine = jnp.cos(phase_angle)
    sine_part = jnp.sin(phase_angle)
    real_in = samples[0].astype(jnp.float32)[None, :]
    imag_in = samples[1].astype(jnp.float32)[None, :]
    mixed_real = (real_in * cosine + imag_in * sine_part).astype(jnp.bfloat16)
    mixed_imag = (imag_in * cosine - real_in * sine_part).astype(jnp.bfloat16)
    upper_half = jnp.concatenate([mixed_real, mixed_imag], 1)
    lower_half = jnp.concatenate([mixed_imag, -mixed_real], 1)
    return jnp.concatenate([upper_half, lower_half], 0)

def lag_product(toeplitz, mixed):
    height = toeplitz.shape[1]
    stacked = toeplitz.reshape(2 * height, toeplitz.shape[2])
    return lax.dot_general(stacked, mixed, (((0,), (1,)), ((), ())), preferred_element_type=jnp.float32)

def reference(surveillance, reference_signal):
    signal = surveillance.reshape(2, TIME)
    reference_flat = reference_signal.reshape(2, TIME)
    extended = jnp.concatenate([jnp.zeros((2, LAGS - 1), jnp.bfloat16), reference_flat], 1)
    height = min(512, TIME)
    doppler = jnp.arange(F, dtype=jnp.int32) - F // 2

    def one_step(running, turn_no):
        offset = turn_no * height
        segment = lax.dynamic_slice_in_dim(extended, offset, height + LAGS - 1, 1)[:, ::-1]
        toeplitz = toeplitz_rows(segment, height, LAGS)
        samples = lax.dynamic_slice_in_dim(signal, offset, height, 1)[:, ::-1]
        sample_index = offset + height - 1 - jnp.arange(height, dtype=jnp.int32)
        return (running + lag_product(toeplitz, mix_rows(samples, sample_index, doppler, TIME)), None)
    running, unused = lax.scan(one_step, jnp.zeros((LAGS, 2 * F), jnp.float32), jnp.arange(TIME // height, dtype=jnp.int32))
    return running.reshape(LAGS, 2, F) * (1.0 / math.sqrt(TIME))
```

```python
import math

import jax
import jax.numpy as jnp
import numpy as np
from jax import lax
from jax.experimental import pallas as pl
from jax.experimental.pallas import tpu as pltpu
from jax.sharding import PartitionSpec as P

F = 512
LAGS = 2048
BLOCK = 8192
STRIDED = 2048
GROUP = 4


def tables(window):
    depth = STRIDED
    phases = window // depth
    half = F // 2
    q = np.arange(half, dtype=np.float64) + 0.5
    b = np.arange(depth, dtype=np.float64)
    a = np.arange(phases, dtype=np.float64)
    inner = 2.0 * np.pi / depth * np.mod(b[:, None] * q[None, :], depth)
    waves = np.concatenate([np.cos(inner), np.sin(inner)], 1).astype(jnp.bfloat16)
    outer = 2.0 * np.pi / window * a[:, None] * q[None, :]
    scale = 1.0 / math.sqrt(window)
    turns = (np.stack([np.cos(outer), np.sin(outer)]) * scale).astype(np.float32)
    half_b = np.pi / depth * b[None, :]
    half_a = np.pi / window * a[:, None]
    return waves, turns, half_a, half_b


def kernel(lags, s_ref, r_ref, waves_ref, turns_ref, out_ref, shifted, y0, y1, u0, u1):
    phases, depth = s_ref.shape[1:]
    half = turns_ref.shape[2]
    rows = shifted.shape[2]
    per_eight = 8 // GROUP
    groups = lags // GROUP

    for early in range(8):
        for part in range(2):
            for row in range(0, rows, 8):
                shifted[early, part, row : row + 8, :] = r_ref[
                    part, row + 8 - early : row + 16 - early, :
                ]

    def build(group, y):
        eight = group // per_eight
        first = (group % per_eight) * GROUP
        start = lags - 8 - 8 * eight
        for row in range(0, phases, 16):
            here = pl.ds(pl.multiple_of(start + row, 8), 16)
            for lane in range(0, depth, 256):
                lanes = slice(lane, lane + 256)
                sr = s_ref[0, row : row + 16, lanes]
                si = s_ref[1, row : row + 16, lanes]
                for i in range(GROUP):
                    rr = shifted[first + i, 0, here, lanes]
                    ri = shifted[first + i, 1, here, lanes]
                    at = 2 * i * phases + row
                    y[at : at + 16, lanes] = (sr * rr + si * ri).astype(jnp.bfloat16)
                    at += phases
                    y[at : at + 16, lanes] = (si * rr - sr * ri).astype(jnp.bfloat16)

    def transform(y, u):
        u[...] = jnp.dot(y[...], waves_ref[...], preferred_element_type=jnp.float32)

    def gather_phases(group, u):
        for i in range(GROUP):
            for lane in range(0, half, 128):
                cos_lanes = slice(lane, lane + 128)
                sin_lanes = slice(half + lane, half + lane + 128)
                sums = [jnp.zeros((8, 128), jnp.float32) for _ in range(4)]
                for row in range(0, phases, 8):
                    c = turns_ref[0, row : row + 8, cos_lanes]
                    s = turns_ref[1, row : row + 8, cos_lanes]
                    at = 2 * i * phases + row
                    p1 = u[at : at + 8, cos_lanes]
                    p4 = u[at : at + 8, sin_lanes]
                    p3 = u[at + phases : at + phases + 8, cos_lanes]
                    p2 = u[at + phases : at + phases + 8, sin_lanes]
                    sums[0] += p1 * c - p4 * s
                    sums[1] += p2 * c + p3 * s
                    sums[2] += p3 * c - p2 * s
                    sums[3] += p4 * c + p1 * s
                al, be, ga, de = [jnp.sum(v, axis=0, keepdims=True) for v in sums]
                out_ref[group * GROUP + i, :, cos_lanes] = jnp.concatenate(
                    [al + be, ga - de, al - be, ga + de], 0
                )

    build(0, y0)

    @pl.loop(0, groups // 2)
    def _(pair):
        even = pair * 2
        transform(y0, u0)
        build(even + 1, y1)
        gather_phases(jnp.maximum(even - 1, 0), u1)
        transform(y1, u1)
        build(jnp.minimum(even + 2, groups - 1), y0)
        gather_phases(even, u0)

    gather_phases(groups - 1, u1)


def ambiguity_lags(signal, reference, first_lag, lags, interpret=False):
    window = signal.shape[1]
    depth = STRIDED
    phases = window // depth
    half = F // 2
    waves, turns, half_a, half_b = tables(window)

    strided = signal.reshape(2, depth, phases).transpose(0, 2, 1).astype(jnp.float32)
    ca, sa = [jnp.asarray(f(half_a), jnp.float32) for f in (np.cos, np.sin)]
    cb, sb = [jnp.asarray(f(half_b), jnp.float32) for f in (np.cos, np.sin)]
    c = ca * cb - sa * sb
    s = sa * cb + ca * sb
    turned = jnp.stack(
        [strided[0] * c - strided[1] * s, strided[1] * c + strided[0] * s]
    )

    padded = jnp.pad(reference, ((0, 0), (LAGS, phases)))
    delayed = lax.dynamic_slice_in_dim(
        padded, LAGS - lags - first_lag, window + phases, 1
    )
    near = delayed[:, :window].reshape(2, depth, phases)
    far = delayed[:, phases:].reshape(2, depth, phases)[:, :, :lags]
    columns = jnp.concatenate([near, far], 2).transpose(0, 2, 1).astype(jnp.float32)

    tall = GROUP * 2 * phases
    return pl.pallas_call(
        lambda *refs: kernel(lags, *refs),
        out_shape=jax.ShapeDtypeStruct((lags, 4, half), jnp.float32),
        in_specs=[pl.BlockSpec(memory_space=pltpu.VMEM)] * 4,
        out_specs=pl.BlockSpec(memory_space=pltpu.VMEM),
        scratch_shapes=[
            pltpu.VMEM((8, 2, phases + lags - 8, depth), jnp.float32),
            pltpu.VMEM((tall, depth), jnp.bfloat16),
            pltpu.VMEM((tall, depth), jnp.bfloat16),
            pltpu.VMEM((tall, F), jnp.float32),
            pltpu.VMEM((tall, F), jnp.float32),
        ],
        compiler_params=pltpu.CompilerParams(vmem_limit_bytes=56 * 1024 * 1024),
        interpret=interpret,
    )(turned, columns, jnp.asarray(waves), jnp.asarray(turns))


def everywhere(value):
    shape = value.shape
    times, cuts = lax.axis_size("tm"), lax.axis_size("dop")
    every = lax.all_gather(value, ("tm", "dop"), axis=0, tiled=False)
    every = every.reshape((times, cuts) + shape).transpose(2, 0, 3, 1, 4)
    return every.reshape(2, times * cuts * shape[1] * shape[2])


def on_device(surveillance, reference_signal):
    cuts = lax.axis_size("dop")
    lags = LAGS // (lax.axis_size("tm") * cuts)
    first_lag = (lax.axis_index("tm") * cuts + lax.axis_index("dop")) * lags
    signal = everywhere(surveillance)
    reference = everywhere(reference_signal)
    found = ambiguity_lags(signal, reference, first_lag, lags)
    whole = jnp.concatenate([found[:, 2:, ::-1], found[:, :2, :]], 2)
    return lax.all_to_all(whole, "dop", split_axis=2, concat_axis=0, tiled=True)


def solution(mesh):
    return jax.shard_map(
        on_device,
        mesh=mesh,
        in_specs=(P(None, "tm", "dop"), P(None, "tm", "dop")),
        out_specs=P("tm", None, "dop"),
        check_vma=False,
    )
```

```python
import math

import jax
import jax.numpy as jnp
import numpy as np
from jax import lax
from jax.experimental import pallas as pl
from jax.experimental.pallas import tpu as pltpu
from jax.sharding import PartitionSpec as P

F = 512
LAGS = 2048
BLOCK = 8192
STRIDED = 2048
GROUP = 4


def tables(window):
    depth = STRIDED
    phases = window // depth
    half = F // 2
    q = np.arange(half, dtype=np.float64) + 0.5
    b = np.arange(depth, dtype=np.float64)
    a = np.arange(phases, dtype=np.float64)
    inner = 2.0 * np.pi / depth * np.mod(b[:, None] * q[None, :], depth)
    waves = np.concatenate([np.cos(inner), np.sin(inner)], 1).astype(jnp.bfloat16)
    outer = 2.0 * np.pi / window * a[:, None] * q[None, :]
    scale = 1.0 / math.sqrt(window)
    turns = (np.stack([np.cos(outer), np.sin(outer)]) * scale).astype(np.float32)
    half_b = np.pi / depth * b[None, :]
    half_a = np.pi / window * a[:, None]
    return waves, turns, half_a, half_b


def kernel(lags, s_ref, r_ref, waves_ref, turns_ref, out_ref, shifted, y0, y1, u0, u1):
    phases, depth = s_ref.shape[1:]
    half = turns_ref.shape[2]
    rows = shifted.shape[2]
    per_eight = 8 // GROUP
    groups = lags // GROUP

    @pl.loop(0, 2 * (depth // 512))
    def _(turn):
        part = turn % 2
        lanes = pl.ds(pl.multiple_of(turn // 2 * 512, 512), 512)
        for early in range(8):
            for row in range(0, rows, 8):
                shifted[early, part, row : row + 8, lanes] = r_ref[
                    part, row + 8 - early : row + 16 - early, lanes
                ]

    def build(group, y):
        eight = group // per_eight
        first = (group % per_eight) * GROUP
        start = lags - 8 - 8 * eight
        for row in range(0, phases, 16):
            here = pl.ds(pl.multiple_of(start + row, 8), 16)
            for lane in range(0, depth, 256):
                lanes = slice(lane, lane + 256)
                sr = s_ref[0, row : row + 16, lanes]
                si = s_ref[1, row : row + 16, lanes]
                for i in range(GROUP):
                    rr = shifted[first + i, 0, here, lanes]
                    ri = shifted[first + i, 1, here, lanes]
                    at = 2 * i * phases + row
                    y[at : at + 16, lanes] = (sr * rr + si * ri).astype(jnp.bfloat16)
                    at += phases
                    y[at : at + 16, lanes] = (si * rr - sr * ri).astype(jnp.bfloat16)

    def transform(y, u):
        u[...] = jnp.dot(y[...], waves_ref[...], preferred_element_type=jnp.float32)

    def gather_phases(group, u):
        for i in range(GROUP):
            for lane in range(0, half, 128):
                cos_lanes = slice(lane, lane + 128)
                sin_lanes = slice(half + lane, half + lane + 128)
                sums = [jnp.zeros((8, 128), jnp.float32) for _ in range(4)]
                for row in range(0, phases, 8):
                    c = turns_ref[0, row : row + 8, cos_lanes]
                    s = turns_ref[1, row : row + 8, cos_lanes]
                    at = 2 * i * phases + row
                    p1 = u[at : at + 8, cos_lanes]
                    p4 = u[at : at + 8, sin_lanes]
                    p3 = u[at + phases : at + phases + 8, cos_lanes]
                    p2 = u[at + phases : at + phases + 8, sin_lanes]
                    sums[0] += p1 * c - p4 * s
                    sums[1] += p2 * c + p3 * s
                    sums[2] += p3 * c - p2 * s
                    sums[3] += p4 * c + p1 * s
                al, be, ga, de = [jnp.sum(v, axis=0, keepdims=True) for v in sums]
                out_ref[group * GROUP + i, :, cos_lanes] = jnp.concatenate(
                    [al + be, ga - de, al - be, ga + de], 0
                )

    build(0, y0)

    @pl.loop(0, groups // 2)
    def _(pair):
        even = pair * 2
        transform(y0, u0)
        build(even + 1, y1)
        gather_phases(jnp.maximum(even - 1, 0), u1)
        transform(y1, u1)
        build(jnp.minimum(even + 2, groups - 1), y0)
        gather_phases(even, u0)

    gather_phases(groups - 1, u1)


def ambiguity_lags(signal, reference, first_lag, lags, interpret=False):
    window = signal.shape[1]
    depth = STRIDED
    phases = window // depth
    half = F // 2
    waves, turns, half_a, half_b = tables(window)

    strided = signal.reshape(2, depth, phases).transpose(0, 2, 1).astype(jnp.float32)
    ca, sa = [jnp.asarray(f(half_a), jnp.float32) for f in (np.cos, np.sin)]
    cb, sb = [jnp.asarray(f(half_b), jnp.float32) for f in (np.cos, np.sin)]
    c = ca * cb - sa * sb
    s = sa * cb + ca * sb
    turned = jnp.stack(
        [strided[0] * c - strided[1] * s, strided[1] * c + strided[0] * s]
    )

    padded = jnp.pad(reference, ((0, 0), (LAGS, phases)))
    delayed = lax.dynamic_slice_in_dim(
        padded, LAGS - lags - first_lag, window + phases, 1
    )
    near = delayed[:, :window].reshape(2, depth, phases)
    far = delayed[:, phases:].reshape(2, depth, phases)[:, :, :lags]
    columns = jnp.concatenate([near, far], 2).transpose(0, 2, 1).astype(jnp.float32)

    tall = GROUP * 2 * phases
    return pl.pallas_call(
        lambda *refs: kernel(lags, *refs),
        out_shape=jax.ShapeDtypeStruct((lags, 4, half), jnp.float32),
        in_specs=[pl.BlockSpec(memory_space=pltpu.VMEM)] * 4,
        out_specs=pl.BlockSpec(memory_space=pltpu.VMEM),
        scratch_shapes=[
            pltpu.VMEM((8, 2, phases + lags - 8, depth), jnp.float32),
            pltpu.VMEM((tall, depth), jnp.bfloat16),
            pltpu.VMEM((tall, depth), jnp.bfloat16),
            pltpu.VMEM((tall, F), jnp.float32),
            pltpu.VMEM((tall, F), jnp.float32),
        ],
        compiler_params=pltpu.CompilerParams(vmem_limit_bytes=56 * 1024 * 1024),
        interpret=interpret,
    )(turned, columns, jnp.asarray(waves), jnp.asarray(turns))


def flipped(index, bit):
    weight = 1 << bit
    return index + weight * (1 - 2 * ((index // weight) % 2))


def spread_kernel(orders, cuts, *refs):
    count = len(orders)
    own, every = refs[:count], refs[count : 2 * count]
    send_sems, recv_sems = refs[2 * count :]
    me = lax.axis_index("tm") * cuts + lax.axis_index("dop")

    def place(index):
        return {"tm": index // cuts, "dop": index % cuts}

    barrier = pltpu.get_barrier_semaphore()
    for bit in orders[0]:
        pl.semaphore_signal(
            barrier,
            inc=1,
            device_id=place(flipped(me, bit)),
            device_id_type=pl.DeviceIdType.MESH,
        )
    pl.semaphore_wait(barrier, len(orders[0]))

    def copy(which, source, block, slot, target):
        return pltpu.make_async_remote_copy(
            src_ref=source,
            dst_ref=every[which].at[block],
            send_sem=send_sems.at[which, slot],
            recv_sem=recv_sems.at[which, block],
            device_id=place(target),
            device_id_type=pl.DeviceIdType.MESH,
        )

    sent = []
    held = [[me] for _ in orders]
    landed = [1] * count
    for step in range(len(orders[0])):
        partners = [flipped(me, order[step]) for order in orders]
        for at in range(1 << step):
            for which in range(count):
                block = held[which][at]
                mine = every[which].at[block]
                if at == 0:
                    mine = own[which]
                elif at >= landed[which]:
                    copy(which, mine, block, 0, partners[which]).wait_recv()
                    landed[which] = at + 1
                one = copy(which, mine, block, (1 << step) - 1 + at, partners[which])
                one.start()
                sent.append(one)
        for which, order in enumerate(orders):
            held[which] = held[which] + [flipped(h, order[step]) for h in held[which]]
        if step == 0:
            for which in range(count):
                every[which][pl.ds(me, 1)] = own[which][...][None]
    for which in range(count):
        for at in range(landed[which], len(held[which])):
            block = held[which][at]
            copy(which, own[which], block, 0, flipped(me, 0)).wait_recv()
    for one in sent:
        one.wait_send()


def everywhere(values):
    times, cuts = lax.axis_size("tm"), lax.axis_size("dop")
    devices = times * cuts
    bits = devices.bit_length() - 1
    shape = values[0].shape
    order = list(range(bits))[::-1]
    other = order[:-3] + [order[-2], order[-3], order[-1]]
    rows = shape[0] * shape[1] * shape[2] // 128
    block = jax.ShapeDtypeStruct((devices, rows, 128), values[0].dtype)
    gathered = pl.pallas_call(
        lambda *refs: spread_kernel([order, other], cuts, *refs),
        out_shape=[block] * 2,
        in_specs=[pl.BlockSpec(memory_space=pltpu.VMEM)] * 2,
        out_specs=[pl.BlockSpec(memory_space=pltpu.VMEM)] * 2,
        scratch_shapes=[
            pltpu.SemaphoreType.DMA((2, devices)),
            pltpu.SemaphoreType.DMA((2, devices)),
        ],
        compiler_params=pltpu.CompilerParams(collective_id=0, has_side_effects=True),
    )(*[value.reshape(rows, 128) for value in values])
    return [
        every.reshape((times, cuts) + shape)
        .transpose(2, 0, 3, 1, 4)
        .reshape(2, devices * shape[1] * shape[2])
        for every in gathered
    ]


def on_device(surveillance, reference_signal):
    cuts = lax.axis_size("dop")
    lags = LAGS // (lax.axis_size("tm") * cuts)
    first_lag = (lax.axis_index("tm") * cuts + lax.axis_index("dop")) * lags
    signal, reference = everywhere([surveillance, reference_signal])
    found = ambiguity_lags(signal, reference, first_lag, lags)
    whole = jnp.concatenate([found[:, 2:, ::-1], found[:, :2, :]], 2)
    return lax.all_to_all(whole, "dop", split_axis=2, concat_axis=0, tiled=True)


def solution(mesh):
    return jax.shard_map(
        on_device,
        mesh=mesh,
        in_specs=(P(None, "tm", "dop"), P(None, "tm", "dop")),
        out_specs=P("tm", None, "dop"),
        check_vma=False,
    )
```

```python
import math

import jax
import jax.numpy as jnp
import numpy as np
from jax import lax
from jax.experimental import pallas as pl
from jax.experimental.pallas import tpu as pltpu
from jax.sharding import PartitionSpec as P

F = 512
LAGS = 2048
BLOCK = 8192
STRIDED = 2048
GROUP = 4


def tables(window):
    depth = STRIDED
    phases = window // depth
    half = F // 2
    q = np.arange(half, dtype=np.float64) + 0.5
    b = np.arange(depth, dtype=np.float64)
    a = np.arange(phases, dtype=np.float64)
    inner = 2.0 * np.pi / depth * np.mod(b[:, None] * q[None, :], depth)
    waves = np.concatenate([np.cos(inner), np.sin(inner)], 1).astype(jnp.bfloat16)
    outer = 2.0 * np.pi / window * a[:, None] * q[None, :]
    scale = 1.0 / math.sqrt(window)
    turns = (np.stack([np.cos(outer), np.sin(outer)]) * scale).astype(np.float32)
    half_b = np.pi / depth * b[None, :]
    half_a = np.pi / window * a[:, None]
    return waves, turns, half_a, half_b


def kernel(lags, s_ref, r_ref, waves_ref, turns_ref, out_ref, shifted, y0, y1, u0, u1):
    phases, depth = s_ref.shape[1:]
    half = turns_ref.shape[2]
    rows = shifted.shape[2]
    per_eight = 8 // GROUP
    groups = lags // GROUP

    @pl.loop(0, 2 * (depth // 512))
    def _(turn):
        part = turn % 2
        lanes = pl.ds(pl.multiple_of(turn // 2 * 512, 512), 512)
        for early in range(8):
            for row in range(0, rows, 8):
                shifted[early, part, row : row + 8, lanes] = r_ref[
                    part, row + 8 - early : row + 16 - early, lanes
                ]

    def build(group, y):
        eight = group // per_eight
        first = (group % per_eight) * GROUP
        start = lags - 8 - 8 * eight
        for row in range(0, phases, 16):
            here = pl.ds(pl.multiple_of(start + row, 8), 16)
            for lane in range(0, depth, 256):
                lanes = slice(lane, lane + 256)
                sr = s_ref[0, row : row + 16, lanes]
                si = s_ref[1, row : row + 16, lanes]
                for i in range(GROUP):
                    rr = shifted[first + i, 0, here, lanes]
                    ri = shifted[first + i, 1, here, lanes]
                    at = 2 * i * phases + row
                    y[at : at + 16, lanes] = (sr * rr + si * ri).astype(jnp.bfloat16)
                    at += phases
                    y[at : at + 16, lanes] = (si * rr - sr * ri).astype(jnp.bfloat16)

    def transform(y, u):
        u[...] = jnp.dot(y[...], waves_ref[...], preferred_element_type=jnp.float32)

    def gather_phases(group, u):
        for i in range(GROUP):
            for lane in range(0, half, 128):
                cos_lanes = slice(lane, lane + 128)
                sin_lanes = slice(half + lane, half + lane + 128)
                sums = [jnp.zeros((8, 128), jnp.float32) for _ in range(4)]
                for row in range(0, phases, 8):
                    c = turns_ref[0, row : row + 8, cos_lanes]
                    s = turns_ref[1, row : row + 8, cos_lanes]
                    at = 2 * i * phases + row
                    p1 = u[at : at + 8, cos_lanes]
                    p4 = u[at : at + 8, sin_lanes]
                    p3 = u[at + phases : at + phases + 8, cos_lanes]
                    p2 = u[at + phases : at + phases + 8, sin_lanes]
                    sums[0] += p1 * c - p4 * s
                    sums[1] += p2 * c + p3 * s
                    sums[2] += p3 * c - p2 * s
                    sums[3] += p4 * c + p1 * s
                al, be, ga, de = [jnp.sum(v, axis=0, keepdims=True) for v in sums]
                out_ref[group * GROUP + i, :, cos_lanes] = jnp.concatenate(
                    [al + be, ga - de, al - be, ga + de], 0
                )

    build(0, y0)

    @pl.loop(0, groups // 2)
    def _(pair):
        even = pair * 2
        transform(y0, u0)
        build(even + 1, y1)
        gather_phases(jnp.maximum(even - 1, 0), u1)
        transform(y1, u1)
        build(jnp.minimum(even + 2, groups - 1), y0)
        gather_phases(even, u0)

    gather_phases(groups - 1, u1)


def ambiguity_lags(signal, reference, first_lag, lags, interpret=False):
    window = signal.shape[1]
    depth = STRIDED
    phases = window // depth
    half = F // 2
    waves, turns, half_a, half_b = tables(window)

    strided = signal.reshape(2, depth, phases).transpose(0, 2, 1).astype(jnp.float32)
    ca, sa = [jnp.asarray(f(half_a), jnp.float32) for f in (np.cos, np.sin)]
    cb, sb = [jnp.asarray(f(half_b), jnp.float32) for f in (np.cos, np.sin)]
    c = ca * cb - sa * sb
    s = sa * cb + ca * sb
    turned = jnp.stack(
        [strided[0] * c - strided[1] * s, strided[1] * c + strided[0] * s]
    )

    padded = jnp.pad(reference, ((0, 0), (LAGS, phases)))
    delayed = lax.dynamic_slice_in_dim(
        padded, LAGS - lags - first_lag, window + phases, 1
    )
    near = delayed[:, :window].reshape(2, depth, phases)
    far = delayed[:, phases:].reshape(2, depth, phases)[:, :, :lags]
    columns = jnp.concatenate([near, far], 2).transpose(0, 2, 1).astype(jnp.float32)

    tall = GROUP * 2 * phases
    return pl.pallas_call(
        lambda *refs: kernel(lags, *refs),
        out_shape=jax.ShapeDtypeStruct((lags, 4, half), jnp.float32),
        in_specs=[pl.BlockSpec(memory_space=pltpu.VMEM)] * 4,
        out_specs=pl.BlockSpec(memory_space=pltpu.VMEM),
        scratch_shapes=[
            pltpu.VMEM((8, 2, phases + lags - 8, depth), jnp.float32),
            pltpu.VMEM((tall, depth), jnp.bfloat16),
            pltpu.VMEM((tall, depth), jnp.bfloat16),
            pltpu.VMEM((tall, F), jnp.float32),
            pltpu.VMEM((tall, F), jnp.float32),
        ],
        compiler_params=pltpu.CompilerParams(vmem_limit_bytes=56 * 1024 * 1024),
        interpret=interpret,
    )(turned, columns, jnp.asarray(waves), jnp.asarray(turns))


def flipped(index, bit):
    weight = 1 << bit
    return index + weight * (1 - 2 * ((index // weight) % 2))


def spread_kernel(orders, cuts, *refs):
    count = len(orders)
    own, every = refs[:count], refs[count : 2 * count]
    send_sems, recv_sems = refs[2 * count :]
    me = lax.axis_index("tm") * cuts + lax.axis_index("dop")

    def place(index):
        return {"tm": index // cuts, "dop": index % cuts}

    barrier = pltpu.get_barrier_semaphore()
    for bit in orders[0]:
        pl.semaphore_signal(
            barrier,
            inc=1,
            device_id=place(flipped(me, bit)),
            device_id_type=pl.DeviceIdType.MESH,
        )
    pl.semaphore_wait(barrier, len(orders[0]))

    def copy(which, source, block, slot, target):
        return pltpu.make_async_remote_copy(
            src_ref=source,
            dst_ref=every[which].at[block],
            send_sem=send_sems.at[which, slot],
            recv_sem=recv_sems.at[which, block],
            device_id=place(target),
            device_id_type=pl.DeviceIdType.MESH,
        )

    sent = []
    held = [[me] for _ in orders]
    landed = [1] * count
    for step in range(len(orders[0])):
        partners = [flipped(me, order[step]) for order in orders]
        for at in range(1 << step):
            for which in range(count):
                block = held[which][at]
                mine = every[which].at[block]
                if at == 0:
                    mine = own[which]
                elif at >= landed[which]:
                    copy(which, mine, block, 0, partners[which]).wait_recv()
                    landed[which] = at + 1
                one = copy(which, mine, block, (1 << step) - 1 + at, partners[which])
                one.start()
                sent.append(one)
        for which, order in enumerate(orders):
            held[which] = held[which] + [flipped(h, order[step]) for h in held[which]]
        if step == 0:
            for which in range(count):
                every[which][pl.ds(me, 1)] = own[which][...][None]
    for which in range(count):
        for at in range(landed[which], len(held[which])):
            block = held[which][at]
            copy(which, own[which], block, 0, flipped(me, 0)).wait_recv()
    for one in sent:
        one.wait_send()


def everywhere(values):
    times, cuts = lax.axis_size("tm"), lax.axis_size("dop")
    devices = times * cuts
    bits = devices.bit_length() - 1
    shape = values[0].shape
    order = list(range(bits))[::-1]
    other = order[:-3] + [order[-2], order[-3], order[-1]]
    rows = shape[0] * shape[1] * shape[2] // 128
    block = jax.ShapeDtypeStruct((devices, rows, 128), values[0].dtype)
    gathered = pl.pallas_call(
        lambda *refs: spread_kernel([order, other], cuts, *refs),
        out_shape=[block] * 2,
        in_specs=[pl.BlockSpec(memory_space=pltpu.VMEM)] * 2,
        out_specs=[pl.BlockSpec(memory_space=pltpu.VMEM)] * 2,
        scratch_shapes=[
            pltpu.SemaphoreType.DMA((2, devices)),
            pltpu.SemaphoreType.DMA((2, devices)),
        ],
        compiler_params=pltpu.CompilerParams(collective_id=0, has_side_effects=True),
    )(*[value.reshape(rows, 128) for value in values])
    return [
        every.reshape((times, cuts) + shape)
        .transpose(2, 0, 3, 1, 4)
        .reshape(2, devices * shape[1] * shape[2])
        for every in gathered
    ]


def swap_kernel(cuts, parts, out, send_sems, recv_sems):
    me = lax.axis_index("dop")
    partners = [me]
    for bit in range(cuts.bit_length() - 1):
        partners = partners + [flipped(p, bit) for p in partners]
    partners = partners[1:]

    barrier = pltpu.get_barrier_semaphore()
    for partner in partners:
        pl.semaphore_signal(
            barrier,
            inc=1,
            device_id={"dop": partner},
            device_id_type=pl.DeviceIdType.MESH,
        )
    pl.semaphore_wait(barrier, len(partners))

    def copy(source, target, owner):
        return pltpu.make_async_remote_copy(
            src_ref=parts.at[source],
            dst_ref=out.at[owner],
            send_sem=send_sems.at[target],
            recv_sem=recv_sems.at[owner],
            device_id={"dop": target},
            device_id_type=pl.DeviceIdType.MESH,
        )

    for partner in partners:
        copy(partner, partner, me).start()
    out[pl.ds(me, 1)] = parts[pl.ds(me, 1)]
    for partner in partners:
        copy(partner, partner, partner).wait_recv()
    for partner in partners:
        copy(partner, partner, me).wait_send()


def swapped(whole):
    cuts = lax.axis_size("dop")
    lags, two, bins = whole.shape
    parts = whole.reshape(lags, two, cuts, bins // cuts).transpose(2, 0, 1, 3)
    flat = parts.reshape(cuts, lags * two, bins // cuts)
    out = pl.pallas_call(
        lambda *refs: swap_kernel(cuts, *refs),
        out_shape=jax.ShapeDtypeStruct(flat.shape, flat.dtype),
        in_specs=[pl.BlockSpec(memory_space=pltpu.VMEM)],
        out_specs=pl.BlockSpec(memory_space=pltpu.VMEM),
        scratch_shapes=[
            pltpu.SemaphoreType.DMA((cuts,)),
            pltpu.SemaphoreType.DMA((cuts,)),
        ],
        compiler_params=pltpu.CompilerParams(collective_id=1, has_side_effects=True),
    )(flat)
    return out.reshape(cuts * lags, two, bins // cuts)


def on_device(surveillance, reference_signal):
    cuts = lax.axis_size("dop")
    lags = LAGS // (lax.axis_size("tm") * cuts)
    first_lag = (lax.axis_index("tm") * cuts + lax.axis_index("dop")) * lags
    signal, reference = everywhere([surveillance, reference_signal])
    found = ambiguity_lags(signal, reference, first_lag, lags)
    whole = jnp.concatenate([found[:, 2:, ::-1], found[:, :2, :]], 2)
    return swapped(whole)


def solution(mesh):
    return jax.shard_map(
        on_device,
        mesh=mesh,
        in_specs=(P(None, "tm", "dop"), P(None, "tm", "dop")),
        out_specs=P("tm", None, "dop"),
        check_vma=False,
    )
```
